128 devices in a mesh: ep: 64 (over y, x, z), dp: 2 (over core).
Axes of the slice: x: 4, y: 4, z: 4, core: 2. Of those that a mesh axis runs over, the one named last changes fastest.
Arguments:
- layer_input: bfloat16 [8192, 3584], P('ep'), may hold values from -6 to 6
- out_grad: bfloat16 [8192, 3584], P('ep'), may hold values from -6 to 6
- expert_ids: int32 [8192, 8], P('ep'), may hold values from 0 to 63, all different within a row; in each aligned block of 128 rows (0 to 127, 128 to 255, ...) at most 20 rows name the same one
- gate_probs: float32 [8192, 8], P('ep'), may hold values from 0.1 to 1
- gate_proj: bfloat16 [64, 3584, 1024], P('ep'), may hold values from -0.09375 to 0.09375
- up_proj: bfloat16 [64, 3584, 1024], P('ep'), may hold values from -0.09375 to 0.09375
- down_proj: bfloat16 [64, 1024, 3584], P('ep'), may hold values from -0.1875 to 0.1875
Outputs:
- input_grad: bfloat16 [8192, 3584], P('ep', 'dp')
The draws below stay inside these ranges and needn't reach their ends.
Inputs may be any that keep to these rules, and one draw needn't show every extreme that they name: `expert_ids`: each row names 8 different experts. The 128 rows of one device name one expert at most 20 times, and in every draw some device's rows name some expert exactly 20 times.
All inputs are finite; a program needn't handle non-finite values.
Results may differ from the reference program's by a relative error of at most 0.0058.
Values may be sent and summed in bfloat16 or wider, within the bound.
No kernel may reach another device: no remote copies, remote signals or barrier semaphores. Data moves between devices by JAX's collectives and lax.ppermute only.
A program may use at most 192 MiB of HBM per device.

```python
import math
import jax
import jax.numpy as jnp
import numpy as np
from jax import lax

D = 3584
FF = 1024
TOP = 8
TOK_DEV = 128
EXPERTS = 64
CAP = 20
TOKENS = 8192
N_EP = 64


def level_of(rng, extent, shards, least, high):
    gain, own = 1.0, jax.random.fold_in(rng, 6)
    for dim, parts in shards:
        heights = jnp.exp(jax.random.uniform(jax.random.fold_in(own, dim), (parts,), jnp.float32, least / len(shards), high / len(shards)))
        gain = gain * jnp.repeat(heights, extent[dim] // parts).reshape([-1 if axis == dim else 1 for axis in range(len(extent))])
    return gain


def assign_block(rng, own, number, rows, amount, top, limit, lean):
    order = jax.random.permutation(rng, amount)
    packed, usual = portions_of(amount, rows * top, limit, lean, True), portions_of(amount, rows * top, limit, lean, False)
    places = jnp.arange(amount)

    def named(sizes, turn):
        used = int((sizes > 0).sum())
        fixed = max(1, used // 4)
        moved = fixed + (places - fixed + turn * (used - fixed)) % max(1, amount - fixed)
        return jnp.zeros((amount,), jnp.int32).at[order[jnp.where(places < fixed, places, moved)]].set(jnp.asarray(sizes, jnp.int32))

    sizes = jnp.where(number % 4 == 0, named(packed, number // 4), named(usual, number - number // 4 - 1))
    mixed = jax.random.permutation(jax.random.fold_in(own, 3), amount)
    donor, sink = mixed[0:amount // 2 * 2:2], mixed[1:amount // 2 * 2:2]
    room = jnp.minimum(sizes[donor] - 1, limit - sizes[sink]) // 2
    room = jnp.where((donor == order[0]) | (sink == order[0]) | (sizes[sink] == 0), 0, jnp.maximum(room, 0))
    moved = jax.random.randint(jax.random.fold_in(own, 4), (amount // 2,), 0, 1 << 20) % (room + 1)
    sizes = sizes.at[donor].add(-moved).at[sink].add(moved)
    labels = jnp.searchsorted(jnp.cumsum(sizes), jnp.arange(rows * top), side="right").astype(jnp.int32)
    listing = labels.reshape(top, rows).T
    listing = listing[jax.random.permutation(jax.random.fold_in(own, 1), rows)]
    turn = jax.random.randint(jax.random.fold_in(own, 2), (rows, 1), 0, top)
    return jnp.take_along_axis(listing, (jnp.arange(top)[None, :] + turn) % top, axis=1)


def portions_of(number_of, total, reach, slope, full):
    weights = [(1 << 20) // math.isqrt(rank ** slope) + 1 for rank in range(1, number_of + 1)]
    largest = reach if full else min(reach, max(-(-total // number_of), total * weights[0] // sum(weights)))
    least = 1 if total - largest >= number_of - 1 else 0
    given, surplus = [largest] + [least] * (number_of - 1), total - largest - least * (number_of - 1)
    while surplus > 0:
        movable = [i for i in range(1, number_of) if given[i] < largest] or [i for i in range(1, number_of) if given[i] < reach]
        whole, budget = sum([weights[i] for i in movable]), surplus
        for i in movable:
            extra = min(reach - given[i], max(1, budget * weights[i] // whole), surplus)
            given[i] = given[i] + extra
            surplus = surplus - extra
    return np.array(given)


def bell_draw(stream_key, extent, deviation, most, pieces=(), kind=jnp.bfloat16):
    drawn = jax.random.normal(stream_key, extent, jnp.float32) * deviation
    if len(pieces) > 0:
        drawn = level_of(stream_key, extent, pieces, -0.22, 0.18) * drawn
    return jnp.clip(drawn, min=-most, max=most).astype(kind)


def setup_inputs(seed: int = 0) -> dict:
    streams_of = jax.random.split(jax.random.key(seed), 8)
    layer_input = bell_draw(streams_of[0], (TOKENS, D), 1.0, 6.0, ((0, 64),))
    out_grad = bell_draw(streams_of[1], (TOKENS, D), 1.0, 6.0, ((0, 64),))
    expert_ids_keys = jax.random.split(jax.random.fold_in(streams_of[2], 1), TOKENS // TOK_DEV)
    expert_ids_turns = jax.random.permutation(jax.random.fold_in(streams_of[2], 3), TOKENS // TOK_DEV)
    expert_ids = jax.vmap(lambda own, number: assign_block(jax.random.fold_in(streams_of[2], 2), own, number, TOK_DEV, EXPERTS, TOP, CAP, 1))(expert_ids_keys, expert_ids_turns).reshape((TOKENS, TOP))
    gate_probs = jnp.clip(0.1 + 0.9 * jax.random.uniform(streams_of[3], (TOKENS, TOP), jnp.float32) ** level_of(streams_of[3], (TOKENS, TOP), ((0, 64),), -0.2, 0.2), 0.1, 1.0)
    gate_proj = bell_draw(streams_of[4], (EXPERTS, D, FF), D ** -0.5, 0.09375, ((0, 64),))
    up_proj = bell_draw(streams_of[5], (EXPERTS, D, FF), D ** -0.5, 0.09375, ((0, 64),))
    down_proj = bell_draw(streams_of[6], (EXPERTS, FF, D), FF ** -0.5, 0.1875, ((0, 64),))
    return {"layer_input": layer_input, "out_grad": out_grad, "expert_ids": expert_ids, "gate_probs": gate_probs, "gate_proj": gate_proj, "up_proj": up_proj, "down_proj": down_proj}


def slot_ranks(flat_ids, experts_count):
    onehot = (flat_ids[:, None] == jnp.arange(experts_count, dtype=jnp.int32)[None, :]).astype(jnp.int32)
    running = jnp.cumsum(onehot, axis=0)
    return jnp.sum((running - 1) * onehot, axis=1).astype(jnp.int32)


def expert_backward(in_rows, grad_rows, gate_mat, up_mat, down_mat):
    gate_pre = jnp.dot(in_rows, gate_mat, preferred_element_type=jnp.float32)
    up_pre = jnp.dot(in_rows, up_mat, preferred_element_type=jnp.float32)
    hidden_grad = lax.dot_general(grad_rows, down_mat, (((1,), (1,)), ((), ())), preferred_element_type=jnp.float32)
    sigmoid = jax.nn.sigmoid(gate_pre)
    gate_grad = (hidden_grad * up_pre * sigmoid * (1.0 + gate_pre * (1.0 - sigmoid))).astype(jnp.bfloat16)
    up_grad = (hidden_grad * gate_pre * sigmoid).astype(jnp.bfloat16)
    back_gate = lax.dot_general(gate_grad, gate_mat, (((1,), (1,)), ((), ())), preferred_element_type=jnp.float32)
    back_up = lax.dot_general(up_grad, up_mat, (((1,), (1,)), ((), ())), preferred_element_type=jnp.float32)
    return back_gate + back_up


def reference(layer_input, out_grad, expert_ids, gate_probs, gate_proj, up_proj, down_proj):
    features = layer_input.shape[1]
    per_dev = TOK_DEV * TOP
    blocks = expert_ids.reshape(N_EP, per_dev).astype(jnp.int32)
    slot_rank = jax.vmap(lambda flat_ids: slot_ranks(flat_ids, EXPERTS))(blocks)
    source = jnp.arange(N_EP, dtype=jnp.int32)[:, None]
    token_index = source * TOK_DEV + jnp.arange(per_dev, dtype=jnp.int32)[None, :] // TOP
    column = (source * CAP + slot_rank).astype(jnp.int32)
    slot_token = jnp.full((EXPERTS, N_EP * CAP), TOKENS, jnp.int32).at[blocks, column].set(token_index.astype(jnp.int32))
    slot_prob = jnp.zeros((EXPERTS, N_EP * CAP), jnp.float32).at[blocks, column].set(gate_probs.reshape(N_EP, per_dev).astype(jnp.float32))
    padded_in = jnp.concatenate([layer_input, jnp.zeros((1, features), layer_input.dtype)], 0)
    padded_grad = jnp.concatenate([out_grad, jnp.zeros((1, features), out_grad.dtype)], 0)

    def per_expert(running_sum, expert_items):
        gate_mat, up_mat, down_mat, tokens_here, probs_here = expert_items
        result = expert_backward(padded_in[tokens_here], padded_grad[tokens_here], gate_mat, up_mat, down_mat).astype(jnp.bfloat16)
        running_sum = running_sum.at[tokens_here].add(result.astype(jnp.float32) * probs_here[:, None])
        return running_sum, None

    start_sum = jnp.zeros((TOKENS + 1, features), jnp.float32)
    running_sum, unused = lax.scan(per_expert, start_sum, (gate_proj, up_proj, down_proj, slot_token, slot_prob))
    return running_sum[:TOKENS].astype(jnp.bfloat16)
```

```python
import jax
import jax.numpy as jnp
from jax import lax
from jax.experimental import pallas as pl
from jax.experimental.pallas import tpu as pltpu
from jax.sharding import PartitionSpec as P

BF16, F32 = jnp.bfloat16, jnp.float32
TILE = 8
WIDE, TAIL = 512, 128
STEP = WIDE + TAIL
FOLD = WIDE // TAIL


def iota(shape, dim):
    return lax.broadcasted_iota(jnp.int32, shape, dim)


def slot_keys(ids_ref, base, experts):
    top, tokens = ids_ref.shape
    number = iota((experts, tokens), 0)
    named = ids_ref[0:1, :] == number
    for k in range(1, top):
        named = named | (ids_ref[k : k + 1, :] == number)
    before = jnp.where(iota((tokens, tokens), 0) < iota((tokens, tokens), 1), 1.0, 0.0).astype(BF16)
    rank = jnp.dot(jnp.where(named, 1.0, 0.0).astype(BF16), before, preferred_element_type=F32)
    key = jnp.where(named, rank - base, -100.0).astype(BF16)
    return jnp.dot(spread(experts), key, preferred_element_type=F32)


def spread(experts):
    shape = (experts * TILE, experts)
    return jnp.where(iota(shape, 0) // TILE == iota(shape, 1), 1.0, 0.0).astype(BF16)


def dispatch_kernel(experts, base_ref, ids_ref, x_ref, g_ref, out_ref, main_sel, tail_sel):
    step, half = pl.program_id(0), pl.num_programs(0) // 2
    tokens = ids_ref.shape[1]

    @pl.when(step == 0)
    def _():
        key = slot_keys(ids_ref, base_ref[0].astype(F32), experts)
        row = iota(key.shape, 0) % TILE
        main_sel[...] = jnp.where(key == row.astype(F32), 1.0, 0.0).astype(BF16)
        late = key == (TILE + row % 2).astype(F32)
        for q in range(FOLD):
            tail_sel[:, q * tokens : (q + 1) * tokens] = jnp.where(late & (row // 2 == q), 1.0, 0.0).astype(BF16)

    def put(ref):
        block = ref[...]
        out_ref[:, 0:WIDE] = jnp.dot(main_sel[...], block, preferred_element_type=F32).astype(BF16)
        parts = jnp.concatenate([block[:, q * TAIL : (q + 1) * TAIL] for q in range(FOLD)], 0)
        out_ref[:, WIDE:STEP] = jnp.dot(tail_sel[...], parts, preferred_element_type=F32).astype(BF16)

    @pl.when(step < half)
    def _():
        put(x_ref)

    @pl.when(step >= half)
    def _():
        put(g_ref)


def dispatch(base, ids, x, g, experts):
    tokens, features = x.shape
    blocks = features // WIDE
    rows = experts * TILE
    return pl.pallas_call(
        lambda *refs: dispatch_kernel(experts, *refs),
        grid=(2 * blocks,),
        in_specs=[
            pl.BlockSpec(memory_space=pltpu.SMEM),
            pl.BlockSpec(ids.shape, lambda s: (0, 0)),
            pl.BlockSpec((tokens, WIDE), lambda s: (0, jnp.minimum(s, blocks - 1))),
            pl.BlockSpec((tokens, WIDE), lambda s: (0, jnp.maximum(s - blocks, 0))),
        ],
        out_specs=pl.BlockSpec((rows, STEP), lambda s: (0, s)),
        out_shape=jax.ShapeDtypeStruct((rows, 2 * blocks * STEP), BF16),
        scratch_shapes=[pltpu.VMEM((rows, tokens), BF16), pltpu.VMEM((rows, FOLD * tokens), BF16)],
        name="dispatch",
    )(base, ids, x, g)


def weights_kernel(experts, base_ref, ids_ref, probs_ref, main_ref, tail_ref):
    top, tokens = ids_ref.shape
    key = slot_keys(ids_ref, base_ref[0].astype(F32), experts)
    number = iota((experts, tokens), 0)
    prob = jnp.zeros((experts, tokens), F32)
    for k in range(top):
        prob = prob + jnp.where(ids_ref[k : k + 1, :] == number, probs_ref[k : k + 1, :], 0.0)
    high = prob.astype(BF16)
    low = (prob - high.astype(F32)).astype(BF16)
    row = iota(key.shape, 0) % TILE
    main, late = key == row.astype(F32), key == (TILE + row % 2).astype(F32)
    for n, part in enumerate((high, low)):
        wide = jnp.dot(spread(experts), part, preferred_element_type=F32)
        main_ref[n * tokens : (n + 1) * tokens, :] = jnp.where(main, wide, 0.0).T.astype(BF16)
        for q in range(FOLD):
            at = (2 * q + n) * tokens
            tail_ref[at : at + tokens, :] = jnp.where(late & (row // 2 == q), wide, 0.0).T.astype(BF16)


def combine_weights(base, ids, probs, experts):
    tokens = ids.shape[1]
    rows = experts * TILE
    return pl.pallas_call(
        lambda *refs: weights_kernel(experts, *refs),
        in_specs=[
            pl.BlockSpec(memory_space=pltpu.SMEM),
            pl.BlockSpec(memory_space=pltpu.VMEM),
            pl.BlockSpec(memory_space=pltpu.VMEM),
        ],
        out_shape=[
            jax.ShapeDtypeStruct((2 * tokens, rows), BF16),
            jax.ShapeDtypeStruct((2 * FOLD * tokens, rows), BF16),
        ],
        name="combine_weights",
    )(base, ids, probs)


def unfold_matrix(rows, transposed):
    sources = rows // TILE
    unfolded, packed = iota((rows, rows), int(transposed)), iota((rows, rows), 1 - int(transposed))
    per = 2 * sources
    q, rest = unfolded // per, unfolded % per
    at = (rest // 2) * TILE + 2 * q + rest % 2
    return jnp.where(at == packed, 1.0, 0.0).astype(BF16)


def expert_kernel(chunks, packet_ref, gate_cols, up_cols, down_rows, gate_rows, up_rows, out_ref, x_s, g_s, tail_s, gg_s, ug_s, fold_s, sems):
    step = pl.program_id(0)
    rows = packet_ref.shape[0]
    late = rows // FOLD
    blocks = x_s.shape[1] // WIDE

    @pl.when(step == 0)
    def _():
        copies = []
        for n, dst in enumerate((x_s, g_s)):
            for j in range(blocks):
                at = (n * blocks + j) * STEP
                copies.append(pltpu.make_async_copy(packet_ref.at[:, at : at + WIDE], dst.at[0:rows, j * WIDE : (j + 1) * WIDE], sems.at[n]))
                copies.append(pltpu.make_async_copy(packet_ref.at[:, at + WIDE : at + STEP], tail_s.at[n, :, j * TAIL : (j + 1) * TAIL], sems.at[n]))
        for copy in copies:
            copy.start()
        unfold = unfold_matrix(rows, False)
        fold_s[...] = unfold_matrix(rows, True)
        for n, dst in enumerate((x_s, g_s)):
            for copy in copies[n * 2 * blocks : (n + 1) * 2 * blocks]:
                copy.wait()
            tail = jnp.dot(unfold, tail_s[n], preferred_element_type=F32).astype(BF16)
            for q in range(FOLD):
                for j in range(blocks):
                    dst[rows : rows + late, j * WIDE + q * TAIL : j * WIDE + (q + 1) * TAIL] = tail[q * late : (q + 1) * late, j * TAIL : (j + 1) * TAIL]

    @pl.when(step < chunks)
    def _():
        gate_pre = jnp.dot(x_s[...], gate_cols[...], preferred_element_type=F32)
        up_pre = jnp.dot(x_s[...], up_cols[...], preferred_element_type=F32)
        hidden_grad = lax.dot_general(g_s[...], down_rows[...], (((1,), (1,)), ((), ())), preferred_element_type=F32)
        sigmoid = jax.nn.sigmoid(gate_pre)
        common = hidden_grad * sigmoid
        gg_s[step] = (common * up_pre * (1.0 + gate_pre * (1.0 - sigmoid))).astype(BF16)
        ug_s[step] = (common * gate_pre).astype(BF16)

    @pl.when(step >= chunks)
    def _():
        width = gg_s.shape[2]
        gg = jnp.concatenate([gg_s[c] for c in range(chunks)], 1)
        ug = jnp.concatenate([ug_s[c] for c in range(chunks)], 1)
        back = lax.dot_general(gg, gate_rows[...], (((1,), (1,)), ((), ())), preferred_element_type=F32)
        back = back + lax.dot_general(ug, up_rows[...], (((1,), (1,)), ((), ())), preferred_element_type=F32)
        back = back.astype(BF16)
        out_ref[:, 0:WIDE] = back[0:rows]
        parts = jnp.concatenate([back[rows:, q * TAIL : (q + 1) * TAIL] for q in range(FOLD)], 0)
        out_ref[:, WIDE:STEP] = jnp.dot(fold_s[...], parts, preferred_element_type=F32).astype(BF16)


def expert_backward(packets, gate, up, down):
    features, hidden = gate.shape
    rows = packets.shape[0]
    items = rows + rows // FOLD
    blocks = features // WIDE
    width = 256
    chunks = hidden // width
    first = lambda s: jnp.minimum(s, chunks - 1)
    second = lambda s: jnp.maximum(s - chunks, 0)
    return pl.pallas_call(
        lambda *refs: expert_kernel(chunks, *refs),
        grid=(chunks + blocks,),
        in_specs=[
            pl.BlockSpec(memory_space=pl.ANY),
            pl.BlockSpec((features, width), lambda s: (0, first(s))),
            pl.BlockSpec((features, width), lambda s: (0, first(s))),
            pl.BlockSpec((width, features), lambda s: (first(s), 0)),
            pl.BlockSpec((WIDE, hidden), lambda s: (second(s), 0)),
            pl.BlockSpec((WIDE, hidden), lambda s: (second(s), 0)),
        ],
        out_specs=pl.BlockSpec((rows, STEP), lambda s: (0, second(s))),
        out_shape=jax.ShapeDtypeStruct((rows, blocks * STEP), BF16),
        scratch_shapes=[
            pltpu.VMEM((items, features), BF16),
            pltpu.VMEM((items, features), BF16),
            pltpu.VMEM((2, rows, blocks * TAIL), BF16),
            pltpu.VMEM((chunks, items, width), BF16),
            pltpu.VMEM((chunks, items, width), BF16),
            pltpu.VMEM((rows, rows), BF16),
            pltpu.SemaphoreType.DMA((2,)),
        ],
        compiler_params=pltpu.CompilerParams(vmem_limit_bytes=60 * 1024 * 1024),
        name="expert_backward",
    )(packets, gate, up, down, gate, up)


def combine_kernel(main_ref, tail_ref, back_ref, out_ref):
    tokens = out_ref.shape[0]
    both = jnp.dot(main_ref[...], back_ref[:, 0:WIDE], preferred_element_type=F32)
    late = jnp.dot(tail_ref[...], back_ref[:, WIDE:STEP], preferred_element_type=F32)
    for q in range(FOLD):
        cols = slice(q * TAIL, (q + 1) * TAIL)
        at = 2 * q * tokens
        low = both[tokens:, cols] + late[at + tokens : at + 2 * tokens]
        out_ref[:, cols] = both[:tokens, cols] + late[at : at + tokens] + low


def combine(main, tail, back):
    rows, width = back.shape
    blocks = width // STEP
    tokens = main.shape[0] // 2
    return pl.pallas_call(
        combine_kernel,
        grid=(blocks,),
        in_specs=[
            pl.BlockSpec(main.shape, lambda s: (0, 0)),
            pl.BlockSpec(tail.shape, lambda s: (0, 0)),
            pl.BlockSpec((rows, STEP), lambda s: (0, s)),
        ],
        out_specs=pl.BlockSpec((tokens, WIDE), lambda s: (0, s)),
        out_shape=jax.ShapeDtypeStruct((tokens, blocks * WIDE), F32),
        name="combine",
    )(main, tail, back)


def exchange(packets, experts):
    parts = packets.reshape(experts, TILE, -1)
    return lax.all_to_all(parts, "ep", split_axis=0, concat_axis=0, tiled=True).reshape(packets.shape)


def body(layer_input, out_grad, expert_ids, gate_probs, gate_proj, up_proj, down_proj):
    experts = lax.axis_size("ep")
    core = lax.axis_index("dp")
    features = layer_input.shape[1]
    ids = expert_ids.T
    base = jnp.full((1,), (TILE + 2) * core, jnp.int32)
    packets = dispatch(base, ids, layer_input, out_grad, experts)
    arrived = exchange(packets, experts)
    main, tail = combine_weights(base, ids, gate_probs.T, experts)
    back = expert_backward(arrived, gate_proj[0], up_proj[0], down_proj[0])
    returned = exchange(back, experts)
    summed = combine(main, tail, returned)
    half = features // 2
    other = lax.dynamic_slice_in_dim(summed, (1 - core) * half, half, 1)
    own = lax.dynamic_slice_in_dim(summed, core * half, half, 1)
    return (own + lax.ppermute(other, "dp", ((0, 1), (1, 0)))).astype(BF16)


def solution(mesh):
    rows = P("ep", None)
    mats = P("ep", None, None)
    return jax.shard_map(body, mesh=mesh, in_specs=(rows,) * 4 + (mats,) * 3, out_specs=P("ep", "dp"), check_vma=False)
```

```python
import jax
import jax.numpy as jnp
from jax import lax
from jax.experimental import pallas as pl
from jax.experimental.pallas import tpu as pltpu
from jax.sharding import PartitionSpec as P

BF16, F32 = jnp.bfloat16, jnp.float32
TILE = 8
LATE = 2
FOLD = TILE // LATE
TRANSPOSED = (((1,), (1,)), ((), ()))


def iota(shape, dim):
    return lax.broadcasted_iota(jnp.int32, shape, dim)


def dot(a, b):
    return jnp.dot(a, b, preferred_element_type=F32)


def dot_t(a, b):
    return lax.dot_general(a, b, TRANSPOSED, preferred_element_type=F32)


def spread(experts):
    shape = (experts * TILE, experts)
    return jnp.where(iota(shape, 0) // TILE == iota(shape, 1), 1.0, 0.0).astype(BF16)


def slot_keys(ids_ref, core, experts):
    top, tokens = ids_ref.shape
    number = iota((experts, tokens), 0)
    named = ids_ref[0:1, :] == number
    for k in range(1, top):
        named = named | (ids_ref[k : k + 1, :] == number)
    before = jnp.where(iota((tokens, tokens), 0) < iota((tokens, tokens), 1), 1.0, 0.0).astype(BF16)
    rank = dot(jnp.where(named, 1.0, 0.0).astype(BF16), before)
    base = ((TILE + LATE) * core).astype(F32)
    key = jnp.where(named, rank - base, -100.0).astype(BF16)
    return dot(spread(experts), key)


def main_match(key):
    return key == (iota(key.shape, 0) % TILE).astype(F32)


def late_match(key, q):
    row = iota(key.shape, 0) % TILE
    return (key == (TILE + row % LATE).astype(F32)) & (row // LATE == q)


def dispatch_main_kernel(experts, core_ref, ids_ref, x_ref, g_ref, out_ref, select):
    step, half = pl.program_id(0), pl.num_programs(0) // 2

    @pl.when(step == 0)
    def _():
        key = slot_keys(ids_ref, core_ref[0], experts)
        select[...] = jnp.where(main_match(key), 1.0, 0.0).astype(BF16)

    @pl.when(step < half)
    def _():
        out_ref[...] = dot(select[...], x_ref[...]).astype(BF16)

    @pl.when(step >= half)
    def _():
        out_ref[...] = dot(select[...], g_ref[...]).astype(BF16)


def dispatch_main(core, ids, x, g, experts):
    tokens, features = x.shape
    blocks, rows = FOLD, experts * TILE
    width = features // blocks
    return pl.pallas_call(
        lambda *refs: dispatch_main_kernel(experts, *refs),
        grid=(2 * blocks,),
        in_specs=[
            pl.BlockSpec(memory_space=pltpu.SMEM),
            pl.BlockSpec(ids.shape, lambda s: (0, 0)),
            pl.BlockSpec((tokens, width), lambda s: (0, jnp.minimum(s, blocks - 1))),
            pl.BlockSpec((tokens, width), lambda s: (0, jnp.maximum(s - blocks, 0))),
        ],
        out_specs=pl.BlockSpec((rows, width), lambda s: (0, s)),
        out_shape=jax.ShapeDtypeStruct((rows, 2 * features), BF16),
        scratch_shapes=[pltpu.VMEM((rows, tokens), BF16)],
        name="dispatch_main",
    )(core, ids, x, g)


def dispatch_late_kernel(experts, core_ref, ids_ref, x_ref, g_ref, out_ref):
    key = slot_keys(ids_ref, core_ref[0], experts)
    width = out_ref.shape[1] // 2
    select = jnp.concatenate([jnp.where(late_match(key, q), 1.0, 0.0).astype(BF16) for q in range(FOLD)], 1)
    for n, ref in enumerate((x_ref, g_ref)):
        stacked = jnp.concatenate([ref[:, q * width : (q + 1) * width] for q in range(FOLD)], 0)
        out_ref[:, n * width : (n + 1) * width] = dot(select, stacked).astype(BF16)


def dispatch_late(core, ids, x, g, experts):
    features = x.shape[1]
    return pl.pallas_call(
        lambda *refs: dispatch_late_kernel(experts, *refs),
        in_specs=[pl.BlockSpec(memory_space=pltpu.SMEM)] + [pl.BlockSpec(memory_space=pltpu.VMEM)] * 3,
        out_shape=jax.ShapeDtypeStruct((experts * TILE, 2 * features // FOLD), BF16),
        name="dispatch_late",
    )(core, ids, x, g)


def weights_kernel(experts, core_ref, ids_ref, probs_ref, main_ref, late_ref):
    top, tokens = ids_ref.shape
    key = slot_keys(ids_ref, core_ref[0], experts)
    number = iota((experts, tokens), 0)
    prob = jnp.zeros((experts, tokens), F32)
    for k in range(top):
        prob = prob + jnp.where(ids_ref[k : k + 1, :] == number, probs_ref[k : k + 1, :], 0.0)
    high = prob.astype(BF16)
    low = (prob - high.astype(F32)).astype(BF16)
    for n, part in enumerate((high, low)):
        wide = dot(spread(experts), part)
        main_ref[n * tokens : (n + 1) * tokens, :] = jnp.where(main_match(key), wide, 0.0).T.astype(BF16)
        for q in range(FOLD):
            at = (2 * q + n) * tokens
            late_ref[at : at + tokens, :] = jnp.where(late_match(key, q), wide, 0.0).T.astype(BF16)


def combine_weights(core, ids, probs, experts):
    tokens = ids.shape[1]
    rows = experts * TILE
    return pl.pallas_call(
        lambda *refs: weights_kernel(experts, *refs),
        in_specs=[pl.BlockSpec(memory_space=pltpu.SMEM)] + [pl.BlockSpec(memory_space=pltpu.VMEM)] * 2,
        out_shape=[
            jax.ShapeDtypeStruct((2 * tokens, rows), BF16),
            jax.ShapeDtypeStruct((2 * FOLD * tokens, rows), BF16),
        ],
        name="combine_weights",
    )(core, ids, probs)


def gradients(gate_pre, up_pre, hidden_grad):
    sigmoid = jax.nn.sigmoid(gate_pre)
    common = hidden_grad * sigmoid
    return (common * up_pre * (1.0 + gate_pre * (1.0 - sigmoid))).astype(BF16), (common * gate_pre).astype(BF16)


def expert_main_kernel(chunks, x_ref, g_ref, gate_cols, up_cols, down_rows, gate_rows, up_rows, out_ref, gg_s, ug_s):
    step = pl.program_id(0)

    @pl.when(step < chunks)
    def _():
        gate_pre = dot(x_ref[...], gate_cols[...])
        up_pre = dot(x_ref[...], up_cols[...])
        hidden_grad = dot_t(g_ref[...], down_rows[...])
        gg_s[step], ug_s[step] = gradients(gate_pre, up_pre, hidden_grad)

    @pl.when(step >= chunks)
    def _():
        gg = jnp.concatenate([gg_s[c] for c in range(chunks)], 1)
        ug = jnp.concatenate([ug_s[c] for c in range(chunks)], 1)
        out_ref[...] = (dot_t(gg, gate_rows[...]) + dot_t(ug, up_rows[...])).astype(BF16)


def expert_main(packets, gate, up, down):
    features, hidden = gate.shape
    rows = packets.shape[0]
    blocks, width = FOLD, 256
    wide, chunks = features // blocks, hidden // width
    first = lambda s: jnp.minimum(s, chunks - 1)
    second = lambda s: jnp.maximum(s - chunks, 0)
    return pl.pallas_call(
        lambda *refs: expert_main_kernel(chunks, *refs),
        grid=(chunks + blocks,),
        in_specs=[
            pl.BlockSpec((rows, features), lambda s: (0, 0), pipeline_mode=pl.Buffered(1)),
            pl.BlockSpec((rows, features), lambda s: (0, 1), pipeline_mode=pl.Buffered(1)),
            pl.BlockSpec((features, width), lambda s: (0, first(s))),
            pl.BlockSpec((features, width), lambda s: (0, first(s))),
            pl.BlockSpec((width, features), lambda s: (first(s), 0)),
            pl.BlockSpec((wide, hidden), lambda s: (second(s), 0)),
            pl.BlockSpec((wide, hidden), lambda s: (second(s), 0)),
        ],
        out_specs=pl.BlockSpec((rows, wide), lambda s: (0, second(s))),
        out_shape=jax.ShapeDtypeStruct((rows, features + wide), BF16),
        scratch_shapes=[pltpu.VMEM((chunks, rows, width), BF16)] * 2,
        compiler_params=pltpu.CompilerParams(vmem_limit_bytes=60 * 1024 * 1024),
        name="expert_main",
    )(packets, packets, gate, up, down, gate, up)


def unfold_matrix(rows, transposed):
    unfolded, packed = iota((rows, rows), int(transposed)), iota((rows, rows), 1 - int(transposed))
    per = rows // FOLD
    q, rest = unfolded // per, unfolded % per
    at = (rest // LATE) * TILE + LATE * q + rest % LATE
    return jnp.where(at == packed, 1.0, 0.0).astype(BF16)


def expert_late_kernel(packet_ref, gate_ref, up_ref, down_ref, held_ref, out_ref, x_s, g_s, total):
    del held_ref
    step, last = pl.program_id(0), pl.num_programs(0) - 1
    rows = packet_ref.shape[0]
    per = rows // FOLD
    wide = out_ref.shape[1]

    @pl.when(step == 0)
    def _():
        unfolded = dot(unfold_matrix(rows, False), packet_ref[...]).astype(BF16)
        for n, dst in enumerate((x_s, g_s)):
            for q in range(FOLD):
                dst[:, q * wide : (q + 1) * wide] = unfolded[q * per : (q + 1) * per, n * wide : (n + 1) * wide]
        total[...] = jnp.zeros_like(total)

    gate_pre = dot(x_s[...], gate_ref[...])
    up_pre = dot(x_s[...], up_ref[...])
    hidden_grad = dot_t(g_s[...], down_ref[...])
    gate_grad, up_grad = gradients(gate_pre, up_pre, hidden_grad)
    total[...] += dot_t(gate_grad, gate_ref[...]) + dot_t(up_grad, up_ref[...])

    @pl.when(step == last)
    def _():
        stacked = jnp.concatenate([total[:, q * wide : (q + 1) * wide].astype(BF16) for q in range(FOLD)], 0)
        out_ref[...] = dot(unfold_matrix(rows, True), stacked).astype(BF16)


def expert_late(packets, gate, up, down, held):
    features, hidden = gate.shape
    rows = packets.shape[0]
    width, wide = 256, features // FOLD
    return pl.pallas_call(
        expert_late_kernel,
        grid=(hidden // width,),
        in_specs=[
            pl.BlockSpec(packets.shape, lambda s: (0, 0)),
            pl.BlockSpec((features, width), lambda s: (0, s)),
            pl.BlockSpec((features, width), lambda s: (0, s)),
            pl.BlockSpec((width, features), lambda s: (s, 0)),
            pl.BlockSpec(memory_space=pl.ANY),
        ],
        out_specs=pl.BlockSpec((rows, wide), lambda s: (0, FOLD)),
        out_shape=jax.ShapeDtypeStruct(held.shape, BF16),
        scratch_shapes=[pltpu.VMEM((rows // FOLD, features), BF16)] * 2 + [pltpu.VMEM((rows // FOLD, features), F32)],
        input_output_aliases={4: 0},
        compiler_params=pltpu.CompilerParams(vmem_limit_bytes=60 * 1024 * 1024),
        name="expert_late",
    )(packets, gate, up, down, held)


def combine_kernel(half_ref, main_ref, late_ref, back_ref, late_back_ref, out_ref):
    del half_ref
    tokens = out_ref.shape[0]
    both = dot(main_ref[...], back_ref[...]) + dot(late_ref[...], late_back_ref[...])
    out_ref[...] = both[:tokens] + both[tokens:]


def combine(half, main, late, back):
    rows, width = back.shape
    wide = width // (FOLD + 1)
    tokens, steps = main.shape[0] // 2, FOLD // 2
    return pl.pallas_call(
        combine_kernel,
        grid_spec=pltpu.PrefetchScalarGridSpec(
            num_scalar_prefetch=1,
            grid=(steps,),
            in_specs=[
                pl.BlockSpec(main.shape, lambda s, half: (0, 0)),
                pl.BlockSpec((2 * tokens, rows), lambda s, half: (steps * half[0] + s, 0)),
                pl.BlockSpec((rows, wide), lambda s, half: (0, steps * half[0] + s)),
                pl.BlockSpec((rows, wide), lambda s, half: (0, FOLD)),
            ],
            out_specs=pl.BlockSpec((tokens, wide), lambda s, half: (0, s)),
        ),
        out_shape=jax.ShapeDtypeStruct((tokens, steps * wide), F32),
        name="combine",
    )(half, main, late, back, back)


def exchange(packets, experts):
    parts = packets.reshape(experts, TILE, -1)
    return lax.all_to_all(parts, "ep", split_axis=0, concat_axis=0, tiled=True).reshape(packets.shape)


def body(layer_input, out_grad, expert_ids, gate_probs, gate_proj, up_proj, down_proj):
    experts = lax.axis_size("ep")
    core = jnp.full((1,), lax.axis_index("dp"), jnp.int32)
    ids = expert_ids.T
    gate, up, down = gate_proj[0], up_proj[0], down_proj[0]
    arrived = exchange(dispatch_main(core, ids, layer_input, out_grad, experts), experts)
    late_arrived = exchange(dispatch_late(core, ids, layer_input, out_grad, experts), experts)
    main, late = combine_weights(core, ids, gate_probs.T, experts)
    back = expert_late(late_arrived, gate, up, down, expert_main(arrived, gate, up, down))
    returned = exchange(back, experts)
    crossing = lax.ppermute(combine(1 - core, main, late, returned), "dp", ((0, 1), (1, 0)))
    return (combine(core, main, late, returned) + crossing).astype(BF16)


def solution(mesh):
    rows = P("ep", None)
    mats = P("ep", None, None)
    return jax.shard_map(body, mesh=mesh, in_specs=(rows,) * 4 + (mats,) * 3, out_specs=P("ep", "dp"), check_vma=False)
```

```python
import jax
import jax.numpy as jnp
from jax import lax
from jax.experimental import pallas as pl
from jax.experimental.pallas import tpu as pltpu
from jax.sharding import PartitionSpec as P

BF16, F32 = jnp.bfloat16, jnp.float32
TILE = 8
LATE = 2
FOLD = TILE // LATE
WAIT, HOLD = 51500, 17000
VMEM_MIB = 58
TRANSPOSED = (((1,), (1,)), ((), ()))


def iota(shape, dim):
    return lax.broadcasted_iota(jnp.int32, shape, dim)


def dot(a, b):
    return jnp.dot(a, b, preferred_element_type=F32)


def dot_t(a, b):
    return lax.dot_general(a, b, TRANSPOSED, preferred_element_type=F32)


def spread(experts):
    shape = (experts * TILE, experts)
    return jnp.where(iota(shape, 0) // TILE == iota(shape, 1), 1.0, 0.0).astype(BF16)


def slot_keys(ids_ref, core, experts):
    top, tokens = ids_ref.shape
    number = iota((experts, tokens), 0)
    named = ids_ref[0:1, :] == number
    for k in range(1, top):
        named = named | (ids_ref[k : k + 1, :] == number)
    before = jnp.where(iota((tokens, tokens), 0) < iota((tokens, tokens), 1), 1.0, 0.0).astype(BF16)
    rank = dot(jnp.where(named, 1.0, 0.0).astype(BF16), before)
    base = ((TILE + LATE) * core).astype(F32)
    key = jnp.where(named, rank - base, -100.0).astype(BF16)
    return dot(spread(experts), key)


def main_match(key):
    return key == (iota(key.shape, 0) % TILE).astype(F32)


def late_match(key, q):
    row = iota(key.shape, 0) % TILE
    return (key == (TILE + row % LATE).astype(F32)) & (row // LATE == q)


def dispatch_kernel(experts, core_ref, ids_ref, x_ref, g_ref, out_ref, ready, sems):
    key = slot_keys(ids_ref, core_ref[0], experts)
    slots, _, width = ready.shape
    main = jnp.where(main_match(key), 1.0, 0.0).astype(BF16)
    late = jnp.concatenate([jnp.where(late_match(key, q), 1.0, 0.0).astype(BF16) for q in range(FOLD)], 1)
    copies = []
    for ref in (x_ref, g_ref):
        parts = [ref[:, q * width : (q + 1) * width] for q in range(FOLD)]
        for select, rows in [(main, part) for part in parts] + [(late, jnp.concatenate(parts, 0))]:
            n = len(copies)
            if n >= slots:
                copies[n - slots].wait()
            ready[n % slots] = dot(select, rows).astype(BF16)
            copies.append(pltpu.make_async_copy(ready.at[n % slots], out_ref.at[:, n * width : (n + 1) * width], sems.at[n % slots]))
            copies[n].start()
    for copy in copies[-slots:]:
        copy.wait()


def dispatch(core, ids, x, g, experts):
    rows, width = experts * TILE, x.shape[1] // FOLD
    slots = 4
    return pl.pallas_call(
        lambda *refs: dispatch_kernel(experts, *refs),
        in_specs=[pl.BlockSpec(memory_space=pltpu.SMEM)] + [pl.BlockSpec(memory_space=pltpu.VMEM)] * 3,
        out_specs=pl.BlockSpec(memory_space=pl.ANY),
        out_shape=jax.ShapeDtypeStruct((rows, 2 * (FOLD + 1) * width), BF16),
        scratch_shapes=[pltpu.VMEM((slots, rows, width), BF16), pltpu.SemaphoreType.DMA((slots,))],
        name="dispatch",
    )(core, ids, x, g)


def combine_weights(experts, core, ids_ref, probs_ref, main_ref, late_ref):
    top, tokens = ids_ref.shape
    key = slot_keys(ids_ref, core, experts)
    number = iota((experts, tokens), 0)
    prob = jnp.zeros((experts, tokens), F32)
    for k in range(top):
        prob = prob + jnp.where(ids_ref[k : k + 1, :] == number, probs_ref[k : k + 1, :], 0.0)
    high = prob.astype(BF16)
    low = (prob - high.astype(F32)).astype(BF16)
    for n, part in enumerate((high, low)):
        wide = dot(spread(experts), part)
        main_ref[n * tokens : (n + 1) * tokens, :] = jnp.where(main_match(key), wide, 0.0).T.astype(BF16)
        for q in range(FOLD):
            at = (2 * q + n) * tokens
            late_ref[at : at + tokens, :] = jnp.where(late_match(key, q), wide, 0.0).T.astype(BF16)


def pause_kernel(experts, turn, nanos, core_ref, ids_ref, probs_ref, *refs):
    main_ref, late_ref, main_s, late_s, sems = refs[-5:]
    core = core_ref[0]

    @pl.when(core == turn)
    def _():
        combine_weights(experts, core, ids_ref, probs_ref, main_s, late_s)
        copies = [
            pltpu.make_async_copy(main_s, main_ref, sems.at[0]),
            pltpu.make_async_copy(late_s, late_ref, sems.at[1]),
        ]
        for copy in copies:
            copy.start()
        for copy in copies:
            copy.wait()
        pl.delay(nanos)


def pause(turn, nanos, core, ids, probs, experts, packets, weights=()):
    tokens, rows = ids.shape[1], experts * TILE
    shapes = [jax.ShapeDtypeStruct((2 * n * tokens, rows), BF16) for n in (1, FOLD)]
    anywhere = pl.BlockSpec(memory_space=pl.ANY)
    return pl.pallas_call(
        lambda *refs: pause_kernel(experts, turn, nanos, *refs),
        in_specs=[pl.BlockSpec(memory_space=pltpu.SMEM)] + [pl.BlockSpec(memory_space=pltpu.VMEM)] * 2 + [anywhere] * (1 + len(weights)),
        out_specs=[anywhere] * 3,
        out_shape=[jax.ShapeDtypeStruct(packets.shape, packets.dtype)] + shapes,
        scratch_shapes=[pltpu.VMEM(shape.shape, BF16) for shape in shapes] + [pltpu.SemaphoreType.DMA((2,))],
        input_output_aliases={3 + n: n for n in range(1 + len(weights))},
        name="pause",
    )(core, ids, probs, packets, *weights)


def gradients(gate_pre, up_pre, hidden_grad):
    sigmoid = jax.nn.sigmoid(gate_pre)
    common = hidden_grad * sigmoid
    return (common * up_pre * (1.0 + gate_pre * (1.0 - sigmoid))).astype(BF16), (common * gate_pre).astype(BF16)


def unfold_matrix(rows, transposed):
    unfolded, packed = iota((rows, rows), int(transposed)), iota((rows, rows), 1 - int(transposed))
    per = rows // FOLD
    q, rest = unfolded // per, unfolded % per
    at = (rest // LATE) * TILE + LATE * q + rest % LATE
    return jnp.where(at == packed, 1.0, 0.0).astype(BF16)


def expert_kernel(chunks, packet_ref, gate_ref, up_ref, down_ref, out_ref, x_s, g_s, tail_s, fold_s, gate_c, up_c, down_c, gate_r, up_r, gg_s, ug_s, late_s, in_sems, col_sems, row_sems):
    step = pl.program_id(0)
    rows = packet_ref.shape[0]
    wide = out_ref.shape[1]
    width = gate_c.shape[2]
    features = FOLD * wide
    per = rows // FOLD

    def packet_copies(n, dst):
        at = n * (features + wide)
        return (
            pltpu.make_async_copy(packet_ref.at[:, at : at + features], dst.at[0:rows, :], in_sems.at[2 * n]),
            pltpu.make_async_copy(packet_ref.at[:, at + features : at + features + wide], tail_s.at[n], in_sems.at[2 * n + 1]),
        )

    def col_copies(c):
        slot, at = c % 2, pl.multiple_of(c * width, width)
        return (
            pltpu.make_async_copy(gate_ref.at[:, pl.ds(at, width)], gate_c.at[slot], col_sems.at[0, slot]),
            pltpu.make_async_copy(up_ref.at[:, pl.ds(at, width)], up_c.at[slot], col_sems.at[1, slot]),
            pltpu.make_async_copy(down_ref.at[pl.ds(at, width), :], down_c.at[slot], col_sems.at[2, slot]),
        )

    def row_copies(q):
        slot, at = q % 2, pl.multiple_of(q * wide, wide)
        return (
            pltpu.make_async_copy(gate_ref.at[pl.ds(at, wide), :], gate_r.at[slot], row_sems.at[0, slot]),
            pltpu.make_async_copy(up_ref.at[pl.ds(at, wide), :], up_r.at[slot], row_sems.at[1, slot]),
        )

    def start(copies):
        for copy in copies:
            copy.start()

    def wait(copies):
        for copy in copies:
            copy.wait()

    @pl.when(step == 0)
    def _():
        x_main, x_tail = packet_copies(0, x_s)
        g_main, g_tail = packet_copies(1, g_s)
        gate_0, up_0, down_0 = col_copies(0)
        start((x_tail, g_tail, x_main, gate_0, up_0, g_main, down_0))
        start(col_copies(1))
        unfold = unfold_matrix(rows, False)
        fold_s[...] = unfold_matrix(rows, True)
        for n, (dst, copy) in enumerate(((x_s, x_tail), (g_s, g_tail))):
            copy.wait()
            tail = dot(unfold, tail_s[n]).astype(BF16)
            for q in range(FOLD):
                dst[rows : rows + per, q * wide : (q + 1) * wide] = tail[q * per : (q + 1) * per]
        wait((x_main, gate_0, up_0))
        gate_pre = dot(x_s[...], gate_c[0])
        up_pre = dot(x_s[...], up_c[0])
        wait((g_main, down_0))
        hidden_grad = dot_t(g_s[...], down_c[0])
        gg_s[0], ug_s[0] = gradients(gate_pre, up_pre, hidden_grad)

    @pl.when((step > 0) & (step < chunks))
    def _():
        @pl.when(step < chunks - 1)
        def _():
            start(col_copies(step + 1))

        @pl.when(step == chunks - 1)
        def _():
            start(row_copies(0))
            start(row_copies(1))

        wait(col_copies(step))
        slot = step % 2
        gate_pre = dot(x_s[...], gate_c[slot])
        up_pre = dot(x_s[...], up_c[slot])
        hidden_grad = dot_t(g_s[...], down_c[slot])
        gg_s[step], ug_s[step] = gradients(gate_pre, up_pre, hidden_grad)

    @pl.when((step >= chunks) & (step < chunks + FOLD))
    def _():
        q = step - chunks
        slot = q % 2
        wait(row_copies(q))
        gg = jnp.concatenate([gg_s[c] for c in range(chunks)], 1)
        ug = jnp.concatenate([ug_s[c] for c in range(chunks)], 1)
        back = (dot_t(gg, gate_r[slot]) + dot_t(ug, up_r[slot])).astype(BF16)
        out_ref[...] = back[0:rows]
        late_s[q] = back[rows:]

        @pl.when(q < FOLD - 2)
        def _():
            start(row_copies(q + 2))

    @pl.when(step == chunks + FOLD)
    def _():
        stacked = jnp.concatenate([late_s[q] for q in range(FOLD)], 0)
        out_ref[...] = dot(fold_s[...], stacked).astype(BF16)


def expert_backward(packets, gate, up, down):
    features, hidden = gate.shape
    rows = packets.shape[0]
    items = rows + rows // FOLD
    width, wide = 256, features // FOLD
    chunks = hidden // width
    return pl.pallas_call(
        lambda *refs: expert_kernel(chunks, *refs),
        grid=(chunks + FOLD + 1,),
        in_specs=[pl.BlockSpec(memory_space=pl.ANY)] * 4,
        out_specs=pl.BlockSpec((rows, wide), lambda s: (0, jnp.maximum(s - chunks, 0))),
        out_shape=jax.ShapeDtypeStruct((rows, features + wide), BF16),
        scratch_shapes=[
            pltpu.VMEM((items, features), BF16),
            pltpu.VMEM((items, features), BF16),
            pltpu.VMEM((2, rows, wide), BF16),
            pltpu.VMEM((rows, rows), BF16),
            pltpu.VMEM((2, features, width), BF16),
            pltpu.VMEM((2, features, width), BF16),
            pltpu.VMEM((2, width, features), BF16),
            pltpu.VMEM((2, wide, hidden), BF16),
            pltpu.VMEM((2, wide, hidden), BF16),
            pltpu.VMEM((chunks, items, width), BF16),
            pltpu.VMEM((chunks, items, width), BF16),
            pltpu.VMEM((FOLD, rows // FOLD, wide), BF16),
            pltpu.SemaphoreType.DMA((4,)),
            pltpu.SemaphoreType.DMA((3, 2)),
            pltpu.SemaphoreType.DMA((2, 2)),
        ],
        compiler_params=pltpu.CompilerParams(vmem_limit_bytes=VMEM_MIB * 1024 * 1024),
        name="expert_backward",
    )(packets, gate, up, down)


def combine_kernel(core_ref, main_ref, late_ref, back_ref, late_back_ref, out_ref):
    del core_ref
    tokens = out_ref.shape[0]
    both = dot(main_ref[...], back_ref[...]) + dot(late_ref[...], late_back_ref[...])
    out_ref[...] = both[:tokens] + both[tokens:]


def combine(core, other, main, late, back):
    rows, width = back.shape
    wide = width // (FOLD + 1)
    tokens, steps = main.shape[0] // 2, FOLD // 2
    first = lambda core: steps * ((1 - core[0]) if other else core[0])
    return pl.pallas_call(
        combine_kernel,
        grid_spec=pltpu.PrefetchScalarGridSpec(
            num_scalar_prefetch=1,
            grid=(steps,),
            in_specs=[
                pl.BlockSpec(main.shape, lambda s, core: (0, 0)),
                pl.BlockSpec((2 * tokens, rows), lambda s, core: (first(core) + s, 0)),
                pl.BlockSpec((rows, wide), lambda s, core: (0, first(core) + s)),
                pl.BlockSpec((rows, wide), lambda s, core: (0, FOLD)),
            ],
            out_specs=pl.BlockSpec((tokens, wide), lambda s, core: (0, s)),
        ),
        out_shape=jax.ShapeDtypeStruct((tokens, steps * wide), F32),
        name="combine",
    )(core, main, late, back, back)


def exchange(packets, experts):
    parts = packets.reshape(experts, TILE, -1)
    return lax.all_to_all(parts, "ep", split_axis=0, concat_axis=0, tiled=True).reshape(packets.shape)


def body(layer_input, out_grad, expert_ids, gate_probs, gate_proj, up_proj, down_proj):
    experts = lax.axis_size("ep")
    core = jnp.full((1,), lax.axis_index("dp"), jnp.int32)
    ids = expert_ids.T
    packets = dispatch(core, ids, layer_input, out_grad, experts)
    probs = gate_probs.T
    packets, *weights = pause(1, WAIT, core, ids, probs, experts, packets)
    arrived, main, late = pause(0, HOLD, core, ids, probs, experts, exchange(packets, experts), weights)
    returned = exchange(expert_backward(arrived, gate_proj[0], up_proj[0], down_proj[0]), experts)
    crossing = lax.ppermute(combine(core, True, main, late, returned), "dp", ((0, 1), (1, 0)))
    return (combine(core, False, main, late, returned) + crossing).astype(BF16)


def solution(mesh):
    rows = P("ep", None)
    mats = P("ep", None, None)
    return jax.shard_map(body, mesh=mesh, in_specs=(rows,) * 4 + (mats,) * 3, out_specs=P("ep", "dp"), check_vma=False)
```

```python
import jax
import jax.numpy as jnp
from jax import lax
from jax.experimental import pallas as pl
from jax.experimental.pallas import tpu as pltpu
from jax.sharding import PartitionSpec as P

BF16, F32 = jnp.bfloat16, jnp.float32
TILE = 8
LATE = 4
FOLD = TILE // LATE
CORES = ((0, True), (TILE + LATE, False))
BLOCKS = 4
WAIT, HOLD = 65500, 0
TRANSPOSED = (((1,), (1,)), ((), ()))
SMEM_SPEC, VMEM_SPEC, ANY_SPEC = (pl.BlockSpec(memory_space=space) for space in (pltpu.SMEM, pltpu.VMEM, pl.ANY))


def iota(shape, dim):
    return lax.broadcasted_iota(jnp.int32, shape, dim)


def dot(a, b):
    return jnp.dot(a, b, preferred_element_type=F32)


def dot_t(a, b):
    return lax.dot_general(a, b, TRANSPOSED, preferred_element_type=F32)


def spread(experts):
    shape = (experts * TILE, experts)
    return jnp.where(iota(shape, 0) // TILE == iota(shape, 1), 1.0, 0.0).astype(BF16)


def slot_keys(ids_ref, base, experts):
    top, tokens = ids_ref.shape
    number = iota((experts, tokens), 0)
    named = ids_ref[0:1, :] == number
    for k in range(1, top):
        named = named | (ids_ref[k : k + 1, :] == number)
    before = jnp.where(iota((tokens, tokens), 0) < iota((tokens, tokens), 1), 1.0, 0.0).astype(BF16)
    rank = dot(jnp.where(named, 1.0, 0.0).astype(BF16), before)
    key = jnp.where(named, rank - float(base), -100.0).astype(BF16)
    return dot(spread(experts), key)


def main_match(key):
    return key == (iota(key.shape, 0) % TILE).astype(F32)


def late_match(key, q):
    row = iota(key.shape, 0) % TILE
    return (key == (TILE + row % LATE).astype(F32)) & (row // LATE == q)


def dispatch_kernel(experts, base, tail, ids_ref, x_ref, g_ref, out_ref, ready, sems):
    key = slot_keys(ids_ref, base, experts)
    slots, _, width = ready.shape
    main = jnp.where(main_match(key), 1.0, 0.0).astype(BF16)
    if tail:
        late = jnp.concatenate([jnp.where(late_match(key, q), 1.0, 0.0).astype(BF16) for q in range(FOLD)], 1)
    copies = []
    for ref in (x_ref, g_ref):
        parts = [ref[:, b * width : (b + 1) * width] for b in range(BLOCKS)]
        todo = [(main, part) for part in parts]
        if tail:
            per = BLOCKS // FOLD
            todo += [(late, jnp.concatenate(parts[b::per], 0)) for b in range(per)]
        for select, rows in todo:
            n = len(copies)
            if n >= slots:
                copies[n - slots].wait()
            ready[n % slots] = dot(select, rows).astype(BF16)
            copies.append(pltpu.make_async_copy(ready.at[n % slots], out_ref.at[:, n * width : (n + 1) * width], sems.at[n % slots]))
            copies[n].start()
    for copy in copies[-slots:]:
        copy.wait()


def dispatch(ids, x, g, experts, base, tail):
    features = x.shape[1]
    rows, slots = experts * TILE, 4
    columns = features + (features // FOLD if tail else 0)
    return pl.pallas_call(
        lambda *refs: dispatch_kernel(experts, base, tail, *refs),
        in_specs=[VMEM_SPEC] * 3,
        out_specs=ANY_SPEC,
        out_shape=jax.ShapeDtypeStruct((rows, 2 * columns), BF16),
        scratch_shapes=[pltpu.VMEM((slots, rows, features // BLOCKS), BF16), pltpu.SemaphoreType.DMA((slots,))],
        name="dispatch",
    )(ids, x, g)


def weights_kernel(experts, base, tail, nanos, ids_ref, probs_ref, packets_ref, *refs):
    top, tokens = ids_ref.shape
    key = slot_keys(ids_ref, base, experts)
    number = iota((experts, tokens), 0)
    prob = jnp.zeros((experts, tokens), F32)
    for k in range(top):
        prob = prob + jnp.where(ids_ref[k : k + 1, :] == number, probs_ref[k : k + 1, :], 0.0)
    high = prob.astype(BF16)
    low = (prob - high.astype(F32)).astype(BF16)
    for n, part in enumerate((high, low)):
        wide = dot(spread(experts), part)
        refs[1][n * tokens : (n + 1) * tokens, :] = jnp.where(main_match(key), wide, 0.0).T.astype(BF16)
        for q in range(FOLD if tail else 0):
            at = (2 * q + n) * tokens
            refs[2][at : at + tokens, :] = jnp.where(late_match(key, q), wide, 0.0).T.astype(BF16)
    if nanos:
        pl.delay(nanos)


def weights_and_wait(nanos, ids, probs, packets, experts, base, tail):
    tokens, rows = ids.shape[1], experts * TILE
    shapes = [jax.ShapeDtypeStruct((2 * n * tokens, rows), BF16) for n in ((1, FOLD) if tail else (1,))]
    return pl.pallas_call(
        lambda *refs: weights_kernel(experts, base, tail, nanos, *refs),
        in_specs=[VMEM_SPEC] * 2 + [ANY_SPEC],
        out_specs=[ANY_SPEC] + [VMEM_SPEC] * len(shapes),
        out_shape=[jax.ShapeDtypeStruct(packets.shape, packets.dtype)] + shapes,
        input_output_aliases={2: 0},
        name="weights_and_wait",
    )(ids, probs, packets)


def gradients(gate_pre, up_pre, hidden_grad):
    sigmoid = jax.nn.sigmoid(gate_pre)
    common = hidden_grad * sigmoid
    return (common * up_pre * (1.0 + gate_pre * (1.0 - sigmoid))).astype(BF16), (common * gate_pre).astype(BF16)


def unfold_matrix(rows, transposed):
    unfolded, packed = iota((rows, rows), int(transposed)), iota((rows, rows), 1 - int(transposed))
    per = rows // FOLD
    q, rest = unfolded // per, unfolded % per
    at = (rest // LATE) * TILE + LATE * q + rest % LATE
    return jnp.where(at == packed, 1.0, 0.0).astype(BF16)


def start(copies):
    for copy in copies:
        copy.start()


def wait(copies):
    for copy in copies:
        copy.wait()


def expert_kernel(chunks, tail, packet_ref, gate_ref, up_ref, down_ref, out_ref, x_s, g_s, gate_c, up_c, down_c, gate_r, up_r, gg_s, ug_s, in_sems, col_sems, row_sems, tail_s=None, fold_s=None, late_s=None):
    step = pl.program_id(0)
    rows = packet_ref.shape[0]
    wide = out_ref.shape[1]
    width = gate_c.shape[2]
    features = BLOCKS * wide
    folded = features // FOLD
    per = rows // FOLD

    def packet_copies(n, dst):
        at = n * (packet_ref.shape[1] // 2)
        main = pltpu.make_async_copy(packet_ref.at[:, at : at + features], dst.at[0:rows, :], in_sems.at[2 * n])
        if not tail:
            return main, None
        at += features
        return main, pltpu.make_async_copy(packet_ref.at[:, at : at + folded], tail_s.at[n], in_sems.at[2 * n + 1])

    def col_copies(c):
        slot, at = c % 2, pl.multiple_of(c * width, width)
        return (
            pltpu.make_async_copy(gate_ref.at[:, pl.ds(at, width)], gate_c.at[slot], col_sems.at[0, slot]),
            pltpu.make_async_copy(up_ref.at[:, pl.ds(at, width)], up_c.at[slot], col_sems.at[1, slot]),
            pltpu.make_async_copy(down_ref.at[pl.ds(at, width), :], down_c.at[slot], col_sems.at[2, slot]),
        )

    def row_copies(q):
        slot, at = q % 2, pl.multiple_of(q * wide, wide)
        return (
            pltpu.make_async_copy(gate_ref.at[pl.ds(at, wide), :], gate_r.at[slot], row_sems.at[0, slot]),
            pltpu.make_async_copy(up_ref.at[pl.ds(at, wide), :], up_r.at[slot], row_sems.at[1, slot]),
        )

    @pl.when(step == 0)
    def _():
        x_main, x_tail = packet_copies(0, x_s)
        g_main, g_tail = packet_copies(1, g_s)
        gate_0, up_0, down_0 = col_copies(0)
        start([x_tail, x_main, gate_0, up_0, g_tail, g_main, down_0] if tail else [x_main, gate_0, up_0, g_main, down_0])
        start(col_copies(1))
        if tail:
            unfold = unfold_matrix(rows, False)
            fold_s[...] = unfold_matrix(rows, True)

        def unpack(n, dst, copy):
            if tail:
                copy.wait()
                opened = dot(unfold, tail_s[n]).astype(BF16)
                for q in range(FOLD):
                    dst[rows : rows + per, q * folded : (q + 1) * folded] = opened[q * per : (q + 1) * per]

        unpack(0, x_s, x_tail)
        wait((x_main, gate_0))
        gate_pre = dot(x_s[...], gate_c[0])
        up_0.wait()
        up_pre = dot(x_s[...], up_c[0])
        unpack(1, g_s, g_tail)
        wait((g_main, down_0))
        hidden_grad = dot_t(g_s[...], down_c[0])
        gg_s[0], ug_s[0] = gradients(gate_pre, up_pre, hidden_grad)

    @pl.when((step > 0) & (step < chunks))
    def _():
        @pl.when(step < chunks - 1)
        def _():
            start(col_copies(step + 1))

        @pl.when(step == chunks - 1)
        def _():
            start(row_copies(0))
            start(row_copies(1))

        wait(col_copies(step))
        slot = step % 2
        gate_pre = dot(x_s[...], gate_c[slot])
        up_pre = dot(x_s[...], up_c[slot])
        hidden_grad = dot_t(g_s[...], down_c[slot])
        gg_s[step], ug_s[step] = gradients(gate_pre, up_pre, hidden_grad)

    @pl.when((step >= chunks) & (step < chunks + BLOCKS))
    def _():
        q = step - chunks
        slot = q % 2
        wait(row_copies(q))
        gg = jnp.concatenate([gg_s[c] for c in range(chunks)], 1)
        ug = jnp.concatenate([ug_s[c] for c in range(chunks)], 1)
        back = (dot_t(gg, gate_r[slot]) + dot_t(ug, up_r[slot])).astype(BF16)
        out_ref[...] = back[0:rows]
        if tail:
            late_s[q] = back[rows:]

        @pl.when(q < BLOCKS - 2)
        def _():
            start(row_copies(q + 2))

    if tail:

        @pl.when(step >= chunks + BLOCKS)
        def _():
            b = step - chunks - BLOCKS
            stacked = jnp.concatenate([late_s[q * (BLOCKS // FOLD) + b] for q in range(FOLD)], 0)
            out_ref[...] = dot(fold_s[...], stacked).astype(BF16)


def expert_backward(packets, gate, up, down, tail, width):
    features, hidden = gate.shape
    rows = packets.shape[0]
    late = rows // FOLD if tail else 0
    folded = features // FOLD if tail else 0
    wide, chunks = features // BLOCKS, hidden // width
    scratch = [
        pltpu.VMEM((rows + late, features), BF16),
        pltpu.VMEM((rows + late, features), BF16),
        pltpu.VMEM((2, features, width), BF16),
        pltpu.VMEM((2, features, width), BF16),
        pltpu.VMEM((2, width, features), BF16),
        pltpu.VMEM((2, wide, hidden), BF16),
        pltpu.VMEM((2, wide, hidden), BF16),
        pltpu.VMEM((chunks, rows + late, width), BF16),
        pltpu.VMEM((chunks, rows + late, width), BF16),
        pltpu.SemaphoreType.DMA((4,)),
        pltpu.SemaphoreType.DMA((3, 2)),
        pltpu.SemaphoreType.DMA((2, 2)),
    ]
    if tail:
        scratch += [
            pltpu.VMEM((2, rows, folded), BF16),
            pltpu.VMEM((rows, rows), BF16),
            pltpu.VMEM((BLOCKS, late, wide), BF16),
        ]
    return pl.pallas_call(
        lambda *refs: expert_kernel(chunks, tail, *refs),
        grid=(chunks + BLOCKS + folded // wide,),
        in_specs=[ANY_SPEC] * 4,
        out_specs=pl.BlockSpec((rows, wide), lambda s: (0, jnp.maximum(s - chunks, 0))),
        out_shape=jax.ShapeDtypeStruct((rows, features + folded), BF16),
        scratch_shapes=scratch,
        compiler_params=pltpu.CompilerParams(vmem_limit_bytes=60 * 1024 * 1024),
        name="expert_backward",
    )(packets, gate, up, down)


def combine_kernel(main_ref, back_ref, *refs):
    out_ref = refs[-1]
    tokens = out_ref.shape[0]
    both = dot(main_ref[...], back_ref[...])
    if len(refs) > 1:
        both = both + dot(refs[0][...], refs[1][...])
    out_ref[...] = both[:tokens] + both[tokens:]


def combine(half, back, main, late=None):
    rows, tokens = back.shape[0], main.shape[0] // 2
    steps = BLOCKS // 2
    wide = back.shape[1] // (BLOCKS if late is None else BLOCKS + BLOCKS // FOLD)
    in_specs = [pl.BlockSpec(main.shape, lambda s: (0, 0)), pl.BlockSpec((rows, wide), lambda s: (0, steps * half + s))]
    args = [main, back]
    if late is not None:
        in_specs += [pl.BlockSpec((2 * tokens, rows), lambda s: (half, 0)), pl.BlockSpec((rows, wide), lambda s: (0, BLOCKS + s))]
        args += [late, back]
    return pl.pallas_call(
        combine_kernel,
        grid=(steps,),
        in_specs=in_specs,
        out_specs=pl.BlockSpec((tokens, wide), lambda s: (0, s)),
        out_shape=jax.ShapeDtypeStruct((tokens, steps * wide), F32),
        name="combine",
    )(*args)


def exchange(packets, experts):
    parts = packets.reshape(experts, TILE, -1)
    return lax.all_to_all(parts, "ep", split_axis=0, concat_axis=0, tiled=True).reshape(packets.shape)


def share(core, experts, ids, probs, x, g, gate, up, down):
    base, tail = CORES[core]
    packets = dispatch(ids, x, g, experts, base, tail)
    if core == 0:
        arrived, *weights = weights_and_wait(HOLD, ids, probs, exchange(packets, experts), experts, base, tail)
    else:
        packets, *weights = weights_and_wait(WAIT, ids, probs, packets, experts, base, tail)
        arrived = exchange(packets, experts)
    returned = exchange(expert_backward(arrived, gate, up, down, tail, 256), experts)
    return combine(1 - core, returned, *weights), combine(core, returned, *weights)


def body(layer_input, out_grad, expert_ids, gate_probs, gate_proj, up_proj, down_proj):
    experts = lax.axis_size("ep")
    args = (expert_ids.T, gate_probs.T, layer_input, out_grad, gate_proj[0], up_proj[0], down_proj[0])
    paths = [lambda *args, core=core: share(core, experts, *args) for core in (0, 1)]
    crossing, own = lax.cond(lax.axis_index("dp") == 0, *paths, *args)
    return (own + lax.ppermute(crossing, "dp", ((0, 1), (1, 0)))).astype(BF16)


def solution(mesh):
    rows = P("ep", None)
    mats = P("ep", None, None)
    return jax.shard_map(body, mesh=mesh, in_specs=(rows,) * 4 + (mats,) * 3, out_specs=P("ep", "dp"), check_vma=False)
```

```python
import jax
import jax.numpy as jnp
from jax import lax
from jax.experimental import pallas as pl
from jax.experimental.pallas import tpu as pltpu
from jax.sharding import PartitionSpec as P

BF16, F32 = jnp.bfloat16, jnp.float32
TILE = 8
LATE = 4
FOLD = TILE // LATE
CORES = ((0, True), (TILE + LATE, False))
BLOCKS = 4
WIDTHS = (512, 256)
WAIT = 64500
TRANSPOSED = (((1,), (1,)), ((), ()))
SMEM_SPEC, VMEM_SPEC, ANY_SPEC = (pl.BlockSpec(memory_space=space) for space in (pltpu.SMEM, pltpu.VMEM, pl.ANY))


def iota(shape, dim):
    return lax.broadcasted_iota(jnp.int32, shape, dim)


def dot(a, b):
    return jnp.dot(a, b, preferred_element_type=F32)


def dot_t(a, b):
    return lax.dot_general(a, b, TRANSPOSED, preferred_element_type=F32)


def spread(experts):
    shape = (experts * TILE, experts)
    return jnp.where(iota(shape, 0) // TILE == iota(shape, 1), 1.0, 0.0).astype(BF16)


def slot_keys(ids_ref, base, experts):
    top, tokens = ids_ref.shape
    number = iota((experts, tokens), 0)
    named = ids_ref[0:1, :] == number
    for k in range(1, top):
        named = named | (ids_ref[k : k + 1, :] == number)
    before = jnp.where(iota((tokens, tokens), 0) < iota((tokens, tokens), 1), 1.0, 0.0).astype(BF16)
    rank = dot(jnp.where(named, 1.0, 0.0).astype(BF16), before)
    key = jnp.where(named, rank - float(base), -100.0).astype(BF16)
    return dot(spread(experts), key)


def main_match(key):
    return key == (iota(key.shape, 0) % TILE).astype(F32)


def late_match(key, q):
    row = iota(key.shape, 0) % TILE
    return (key == (TILE + row % LATE).astype(F32)) & (row // LATE == q)


def dispatch_kernel(experts, base, tail, ids_ref, x_ref, g_ref, out_ref, ready, sems):
    key = slot_keys(ids_ref, base, experts)
    slots, _, width = ready.shape
    main = jnp.where(main_match(key), 1.0, 0.0).astype(BF16)
    if tail:
        late = jnp.concatenate([jnp.where(late_match(key, q), 1.0, 0.0).astype(BF16) for q in range(FOLD)], 1)
    copies = []
    for ref in (x_ref, g_ref):
        parts = [ref[:, b * width : (b + 1) * width] for b in range(BLOCKS)]
        todo = [(main, part) for part in parts]
        if tail:
            per = BLOCKS // FOLD
            todo += [(late, jnp.concatenate(parts[b::per], 0)) for b in range(per)]
        for select, rows in todo:
            n = len(copies)
            if n >= slots:
                copies[n - slots].wait()
            ready[n % slots] = dot(select, rows).astype(BF16)
            copies.append(pltpu.make_async_copy(ready.at[n % slots], out_ref.at[:, n * width : (n + 1) * width], sems.at[n % slots]))
            copies[n].start()
    for copy in copies[-slots:]:
        copy.wait()


def dispatch(ids, x, g, experts, base, tail):
    features = x.shape[1]
    rows, slots = experts * TILE, 4
    columns = features + (features // FOLD if tail else 0)
    return pl.pallas_call(
        lambda *refs: dispatch_kernel(experts, base, tail, *refs),
        in_specs=[VMEM_SPEC] * 3,
        out_specs=ANY_SPEC,
        out_shape=jax.ShapeDtypeStruct((rows, 2 * columns), BF16),
        scratch_shapes=[pltpu.VMEM((slots, rows, features // BLOCKS), BF16), pltpu.SemaphoreType.DMA((slots,))],
        name="dispatch",
    )(ids, x, g)


def weights_kernel(experts, base, tail, nanos, ids_ref, probs_ref, packets_ref, *refs):
    top, tokens = ids_ref.shape
    key = slot_keys(ids_ref, base, experts)
    number = iota((experts, tokens), 0)
    prob = jnp.zeros((experts, tokens), F32)
    for k in range(top):
        prob = prob + jnp.where(ids_ref[k : k + 1, :] == number, probs_ref[k : k + 1, :], 0.0)
    high = prob.astype(BF16)
    low = (prob - high.astype(F32)).astype(BF16)
    for n, part in enumerate((high, low)):
        wide = dot(spread(experts), part)
        refs[1][n * tokens : (n + 1) * tokens, :] = jnp.where(main_match(key), wide, 0.0).T.astype(BF16)
        for q in range(FOLD if tail else 0):
            at = (2 * q + n) * tokens
            refs[2][at : at + tokens, :] = jnp.where(late_match(key, q), wide, 0.0).T.astype(BF16)
    if nanos:
        pl.delay(nanos)


def weights_and_wait(nanos, ids, probs, packets, experts, base, tail):
    tokens, rows = ids.shape[1], experts * TILE
    shapes = [jax.ShapeDtypeStruct((2 * n * tokens, rows), BF16) for n in ((1, FOLD) if tail else (1,))]
    return pl.pallas_call(
        lambda *refs: weights_kernel(experts, base, tail, nanos, *refs),
        in_specs=[VMEM_SPEC] * 2 + [ANY_SPEC],
        out_specs=[ANY_SPEC] + [VMEM_SPEC] * len(shapes),
        out_shape=[jax.ShapeDtypeStruct(packets.shape, packets.dtype)] + shapes,
        input_output_aliases={2: 0},
        name="weights_and_wait",
    )(ids, probs, packets)


def gradients(gate_pre, up_pre, hidden_grad):
    sigmoid = jax.nn.sigmoid(gate_pre)
    common = hidden_grad * sigmoid
    return (common * up_pre * (1.0 + gate_pre * (1.0 - sigmoid))).astype(BF16), (common * gate_pre).astype(BF16)


def unfold_matrix(rows, transposed):
    unfolded, packed = iota((rows, rows), int(transposed)), iota((rows, rows), 1 - int(transposed))
    per = rows // FOLD
    q, rest = unfolded // per, unfolded % per
    at = (rest // LATE) * TILE + LATE * q + rest % LATE
    return jnp.where(at == packed, 1.0, 0.0).astype(BF16)


def start(copies):
    for copy in copies:
        copy.start()


def wait(copies):
    for copy in copies:
        copy.wait()


def expert_kernel(chunks, tail, packet_ref, gate_ref, up_ref, down_ref, out_ref, x_s, g_s, gate_c, up_c, down_c, gate_r, up_r, gg_s, ug_s, in_sems, col_sems, row_sems, tail_s=None, fold_s=None, late_s=None):
    step = pl.program_id(0)
    rows = packet_ref.shape[0]
    wide = out_ref.shape[1]
    width = gate_c.shape[2]
    features = x_s.shape[1]
    blocks = features // wide
    folded = features // FOLD
    per = rows // FOLD

    def packet_copies(n, dst):
        at = n * (packet_ref.shape[1] // 2)
        main = pltpu.make_async_copy(packet_ref.at[:, at : at + features], dst.at[0:rows, :], in_sems.at[2 * n])
        if not tail:
            return main, None
        at += features
        return main, pltpu.make_async_copy(packet_ref.at[:, at : at + folded], tail_s.at[n], in_sems.at[2 * n + 1])

    def col_copies(c):
        slot, at = c % 2, pl.multiple_of(c * width, width)
        return (
            pltpu.make_async_copy(gate_ref.at[:, pl.ds(at, width)], gate_c.at[slot], col_sems.at[0, slot]),
            pltpu.make_async_copy(up_ref.at[:, pl.ds(at, width)], up_c.at[slot], col_sems.at[1, slot]),
            pltpu.make_async_copy(down_ref.at[pl.ds(at, width), :], down_c.at[slot], col_sems.at[2, slot]),
        )

    def row_copies(q):
        slot, at = q % 2, pl.multiple_of(q * wide, wide)
        return (
            pltpu.make_async_copy(gate_ref.at[pl.ds(at, wide), :], gate_r.at[slot], row_sems.at[0, slot]),
            pltpu.make_async_copy(up_ref.at[pl.ds(at, wide), :], up_r.at[slot], row_sems.at[1, slot]),
        )

    @pl.when(step == 0)
    def _():
        x_main, x_tail = packet_copies(0, x_s)
        g_main, g_tail = packet_copies(1, g_s)
        gate_0, up_0, down_0 = col_copies(0)
        start([x_tail, x_main, gate_0, up_0, g_tail, g_main, down_0] if tail else [x_main, gate_0, up_0, g_main, down_0])
        start(col_copies(1))
        if tail:
            unfold = unfold_matrix(rows, False)
            fold_s[...] = unfold_matrix(rows, True)

        def unpack(n, dst, copy):
            if tail:
                copy.wait()
                opened = dot(unfold, tail_s[n]).astype(BF16)
                for q in range(FOLD):
                    dst[rows : rows + per, q * folded : (q + 1) * folded] = opened[q * per : (q + 1) * per]

        unpack(0, x_s, x_tail)
        wait((x_main, gate_0))
        gate_pre = dot(x_s[...], gate_c[0])
        up_0.wait()
        up_pre = dot(x_s[...], up_c[0])
        unpack(1, g_s, g_tail)
        wait((g_main, down_0))
        hidden_grad = dot_t(g_s[...], down_c[0])
        gg_s[0], ug_s[0] = gradients(gate_pre, up_pre, hidden_grad)

    @pl.when((step > 0) & (step < chunks))
    def _():
        @pl.when(step < chunks - 1)
        def _():
            start(col_copies(step + 1))

        @pl.when(step == chunks - 1)
        def _():
            start(row_copies(0))
            start(row_copies(1))

        wait(col_copies(step))
        slot = step % 2
        gate_pre = dot(x_s[...], gate_c[slot])
        up_pre = dot(x_s[...], up_c[slot])
        hidden_grad = dot_t(g_s[...], down_c[slot])
        gg_s[step], ug_s[step] = gradients(gate_pre, up_pre, hidden_grad)

    @pl.when((step >= chunks) & (step < chunks + blocks))
    def _():
        q = step - chunks
        slot = q % 2
        wait(row_copies(q))
        gg = jnp.concatenate([gg_s[c] for c in range(chunks)], 1)
        ug = jnp.concatenate([ug_s[c] for c in range(chunks)], 1)
        back = (dot_t(gg, gate_r[slot]) + dot_t(ug, up_r[slot])).astype(BF16)
        out_ref[...] = back[0:rows]
        if tail:
            late_s[q] = back[rows:]

        @pl.when(q < blocks - 2)
        def _():
            start(row_copies(q + 2))

    if tail:

        @pl.when(step >= chunks + BLOCKS)
        def _():
            b = step - chunks - BLOCKS
            stacked = jnp.concatenate([late_s[q * (BLOCKS // FOLD) + b] for q in range(FOLD)], 0)
            out_ref[...] = dot(fold_s[...], stacked).astype(BF16)


def expert_backward(packets, gate, up, down, tail, width):
    features, hidden = gate.shape
    rows = packets.shape[0]
    late = rows // FOLD if tail else 0
    folded = features // FOLD if tail else 0
    blocks = BLOCKS if tail else 7
    wide, chunks = features // blocks, hidden // width
    scratch = [
        pltpu.VMEM((rows + late, features), BF16),
        pltpu.VMEM((rows + late, features), BF16),
        pltpu.VMEM((2, features, width), BF16),
        pltpu.VMEM((2, features, width), BF16),
        pltpu.VMEM((2, width, features), BF16),
        pltpu.VMEM((2, wide, hidden), BF16),
        pltpu.VMEM((2, wide, hidden), BF16),
        pltpu.VMEM((chunks, rows + late, width), BF16),
        pltpu.VMEM((chunks, rows + late, width), BF16),
        pltpu.SemaphoreType.DMA((4,)),
        pltpu.SemaphoreType.DMA((3, 2)),
        pltpu.SemaphoreType.DMA((2, 2)),
    ]
    if tail:
        scratch += [
            pltpu.VMEM((2, rows, folded), BF16),
            pltpu.VMEM((rows, rows), BF16),
            pltpu.VMEM((BLOCKS, late, wide), BF16),
        ]
    return pl.pallas_call(
        lambda *refs: expert_kernel(chunks, tail, *refs),
        grid=(chunks + blocks + folded // wide,),
        in_specs=[ANY_SPEC] * 4,
        out_specs=pl.BlockSpec((rows, wide), lambda s: (0, jnp.maximum(s - chunks, 0))),
        out_shape=jax.ShapeDtypeStruct((rows, features + folded), BF16),
        scratch_shapes=scratch,
        compiler_params=pltpu.CompilerParams(vmem_limit_bytes=60 * 1024 * 1024),
        name="expert_backward",
    )(packets, gate, up, down)


def combine_kernel(main_ref, back_ref, *refs):
    step, half = pl.program_id(0), pl.num_programs(0) // 2
    other_ref, own_ref = refs[-2:]
    tokens = own_ref.shape[0]
    both = dot(main_ref[...], back_ref[...])
    if len(refs) > 2:
        both = both + dot(refs[0][...], refs[1][...])
    total = both[:tokens] + both[tokens:]

    @pl.when(step < half)
    def _():
        other_ref[...] = total

    @pl.when(step >= half)
    def _():
        own_ref[...] = total


def combine(core, back, main, late=None):
    rows, tokens = back.shape[0], main.shape[0] // 2
    half = BLOCKS // 2
    wide = back.shape[1] // (BLOCKS if late is None else BLOCKS + BLOCKS // FOLD)
    block = (lambda s: s) if core else (lambda s: (s + half) % BLOCKS)
    in_specs = [pl.BlockSpec(main.shape, lambda s: (0, 0)), pl.BlockSpec((rows, wide), lambda s: (0, block(s)))]
    args = [main, back]
    if late is not None:
        in_specs += [
            pl.BlockSpec((2 * tokens, rows), lambda s: (block(s) // half, 0)),
            pl.BlockSpec((rows, wide), lambda s: (0, BLOCKS + s % half)),
        ]
        args += [late, back]
    return pl.pallas_call(
        combine_kernel,
        grid=(BLOCKS,),
        in_specs=in_specs,
        out_specs=[
            pl.BlockSpec((tokens, wide), lambda s: (0, jnp.minimum(s, half - 1))),
            pl.BlockSpec((tokens, wide), lambda s: (0, jnp.maximum(s - half, 0))),
        ],
        out_shape=[jax.ShapeDtypeStruct((tokens, half * wide), F32)] * 2,
        name="combine",
    )(*args)


def exchange(packets, experts):
    parts = packets.reshape(experts, TILE, -1)
    return lax.all_to_all(parts, "ep", split_axis=0, concat_axis=0, tiled=True).reshape(packets.shape)


def share(core, experts, ids, probs, x, g, gate, up, down):
    base, tail = CORES[core]
    packets = dispatch(ids, x, g, experts, base, tail)
    if core == 0:
        arrived = exchange(packets, experts)
    else:
        packets, *weights = weights_and_wait(WAIT, ids, probs, packets, experts, base, tail)
        arrived = exchange(packets, experts)
    returned = exchange(expert_backward(arrived, gate, up, down, tail, WIDTHS[core]), experts)
    if core == 0:
        returned, *weights = weights_and_wait(0, ids, probs, returned, experts, base, tail)
    return tuple(combine(core, returned, *weights))


def body(layer_input, out_grad, expert_ids, gate_probs, gate_proj, up_proj, down_proj):
    experts = lax.axis_size("ep")
    args = (expert_ids.T, gate_probs.T, layer_input, out_grad, gate_proj[0], up_proj[0], down_proj[0])
    paths = [lambda *args, core=core: share(core, experts, *args) for core in (0, 1)]
    crossing, own = lax.cond(lax.axis_index("dp") == 0, *paths, *args)
    return (own + lax.ppermute(crossing, "dp", ((0, 1), (1, 0)))).astype(BF16)


def solution(mesh):
    rows = P("ep", None)
    mats = P("ep", None, None)
    return jax.shard_map(body, mesh=mesh, in_specs=(rows,) * 4 + (mats,) * 3, out_specs=P("ep", "dp"), check_vma=False)
```

```python
import jax
import jax.numpy as jnp
from jax import lax
from jax.experimental import pallas as pl
from jax.experimental.pallas import tpu as pltpu
from jax.sharding import PartitionSpec as P

BF16, F32 = jnp.bfloat16, jnp.float32
TILE = 8
LATE = 4
FOLD = TILE // LATE
CORES = ((0, True), (TILE + LATE, False))
BLOCKS = 4
WIDTHS = (512, 256)
WAIT = 64500
TRANSPOSED = (((1,), (1,)), ((), ()))
SMEM_SPEC, VMEM_SPEC, ANY_SPEC = (pl.BlockSpec(memory_space=space) for space in (pltpu.SMEM, pltpu.VMEM, pl.ANY))


def iota(shape, dim):
    return lax.broadcasted_iota(jnp.int32, shape, dim)


def dot(a, b):
    return jnp.dot(a, b, preferred_element_type=F32)


def dot_t(a, b):
    return lax.dot_general(a, b, TRANSPOSED, preferred_element_type=F32)


def spread(experts):
    shape = (experts * TILE, experts)
    return jnp.where(iota(shape, 0) // TILE == iota(shape, 1), 1.0, 0.0).astype(BF16)


def slot_keys(ids_ref, base, experts):
    top, tokens = ids_ref.shape
    number = iota((experts, tokens), 0)
    named = ids_ref[0:1, :] == number
    for k in range(1, top):
        named = named | (ids_ref[k : k + 1, :] == number)
    before = jnp.where(iota((tokens, tokens), 0) < iota((tokens, tokens), 1), 1.0, 0.0).astype(BF16)
    rank = dot(jnp.where(named, 1.0, 0.0).astype(BF16), before)
    key = jnp.where(named, rank - float(base), -100.0).astype(BF16)
    return dot(spread(experts), key)


def main_match(key):
    return key == (iota(key.shape, 0) % TILE).astype(F32)


def late_match(key, q):
    row = iota(key.shape, 0) % TILE
    return (key == (TILE + row % LATE).astype(F32)) & (row // LATE == q)


def dispatch_kernel(experts, base, tail, ids_ref, x_ref, g_ref, out_ref, ready, sems):
    key = slot_keys(ids_ref, base, experts)
    slots, _, width = ready.shape
    main = jnp.where(main_match(key), 1.0, 0.0).astype(BF16)
    if tail:
        late = jnp.concatenate([jnp.where(late_match(key, q), 1.0, 0.0).astype(BF16) for q in range(FOLD)], 1)
    copies = []
    for ref in (x_ref, g_ref):
        parts = [ref[:, b * width : (b + 1) * width] for b in range(BLOCKS)]
        todo = [(main, part) for part in parts]
        if tail:
            per = BLOCKS // FOLD
            todo += [(late, jnp.concatenate(parts[b::per], 0)) for b in range(per)]
        for select, rows in todo:
            n = len(copies)
            if n >= slots:
                copies[n - slots].wait()
            ready[n % slots] = dot(select, rows).astype(BF16)
            copies.append(pltpu.make_async_copy(ready.at[n % slots], out_ref.at[:, n * width : (n + 1) * width], sems.at[n % slots]))
            copies[n].start()
    for copy in copies[-slots:]:
        copy.wait()


def dispatch(ids, x, g, experts, base, tail):
    features = x.shape[1]
    rows, slots = experts * TILE, 4
    columns = features + (features // FOLD if tail else 0)
    return pl.pallas_call(
        lambda *refs: dispatch_kernel(experts, base, tail, *refs),
        in_specs=[VMEM_SPEC] * 3,
        out_specs=ANY_SPEC,
        out_shape=jax.ShapeDtypeStruct((rows, 2 * columns), BF16),
        scratch_shapes=[pltpu.VMEM((slots, rows, features // BLOCKS), BF16), pltpu.SemaphoreType.DMA((slots,))],
        name="dispatch",
    )(ids, x, g)


def weights_kernel(experts, base, tail, nanos, ids_ref, probs_ref, packets_ref, *refs):
    top, tokens = ids_ref.shape
    key = slot_keys(ids_ref, base, experts)
    number = iota((experts, tokens), 0)
    prob = jnp.zeros((experts, tokens), F32)
    for k in range(top):
        prob = prob + jnp.where(ids_ref[k : k + 1, :] == number, probs_ref[k : k + 1, :], 0.0)
    high = prob.astype(BF16)
    low = (prob - high.astype(F32)).astype(BF16)
    for n, part in enumerate((high, low)):
        wide = dot(spread(experts), part)
        refs[1][n * tokens : (n + 1) * tokens, :] = jnp.where(main_match(key), wide, 0.0).T.astype(BF16)
        for q in range(FOLD if tail else 0):
            at = (2 * q + n) * tokens
            refs[2][at : at + tokens, :] = jnp.where(late_match(key, q), wide, 0.0).T.astype(BF16)
    if nanos:
        pl.delay(nanos)


def weights_and_wait(nanos, ids, probs, packets, experts, base, tail):
    tokens, rows = ids.shape[1], experts * TILE
    shapes = [jax.ShapeDtypeStruct((2 * n * tokens, rows), BF16) for n in ((1, FOLD) if tail else (1,))]
    return pl.pallas_call(
        lambda *refs: weights_kernel(experts, base, tail, nanos, *refs),
        in_specs=[VMEM_SPEC] * 2 + [ANY_SPEC],
        out_specs=[ANY_SPEC] + [VMEM_SPEC] * len(shapes),
        out_shape=[jax.ShapeDtypeStruct(packets.shape, packets.dtype)] + shapes,
        input_output_aliases={2: 0},
        name="weights_and_wait",
    )(ids, probs, packets)


def gradients(gate_pre, up_pre, hidden_grad):
    sigmoid = jax.nn.sigmoid(gate_pre)
    common = hidden_grad * sigmoid
    return (common * up_pre * (1.0 + gate_pre * (1.0 - sigmoid))).astype(BF16), (common * gate_pre).astype(BF16)


def unfold_matrix(rows, transposed):
    unfolded, packed = iota((rows, rows), int(transposed)), iota((rows, rows), 1 - int(transposed))
    per = rows // FOLD
    q, rest = unfolded // per, unfolded % per
    at = (rest // LATE) * TILE + LATE * q + rest % LATE
    return jnp.where(at == packed, 1.0, 0.0).astype(BF16)


def start(copies):
    for copy in copies:
        copy.start()


def wait(copies):
    for copy in copies:
        copy.wait()


def expert_kernel(chunks, tail, packet_ref, gate_ref, up_ref, down_ref, out_ref, x_s, g_s, gate_c, up_c, down_c, gate_r, up_r, gg_s, ug_s, in_sems, col_sems, row_sems, tail_s=None, fold_s=None, late_s=None):
    step = pl.program_id(0)
    rows = packet_ref.shape[0]
    wide = out_ref.shape[1]
    width = gate_c.shape[2]
    features = x_s.shape[1]
    blocks = features // wide
    folded = features // FOLD
    per = rows // FOLD

    def packet_copies(n, dst):
        at = n * (packet_ref.shape[1] // 2)
        main = pltpu.make_async_copy(packet_ref.at[:, at : at + features], dst.at[0:rows, :], in_sems.at[2 * n])
        if not tail:
            return main, None
        at += features
        return main, pltpu.make_async_copy(packet_ref.at[:, at : at + folded], tail_s.at[n], in_sems.at[2 * n + 1])

    def col_copies(c):
        slot, at = c % 2, pl.multiple_of(c * width, width)
        return (
            pltpu.make_async_copy(gate_ref.at[:, pl.ds(at, width)], gate_c.at[slot], col_sems.at[0, slot]),
            pltpu.make_async_copy(up_ref.at[:, pl.ds(at, width)], up_c.at[slot], col_sems.at[1, slot]),
            pltpu.make_async_copy(down_ref.at[pl.ds(at, width), :], down_c.at[slot], col_sems.at[2, slot]),
        )

    def row_copies(q):
        slot, at = q % 2, pl.multiple_of(q * wide, wide)
        return (
            pltpu.make_async_copy(gate_ref.at[pl.ds(at, wide), :], gate_r.at[slot], row_sems.at[0, slot]),
            pltpu.make_async_copy(up_ref.at[pl.ds(at, wide), :], up_r.at[slot], row_sems.at[1, slot]),
        )

    @pl.when(step == 0)
    def _():
        x_main, x_tail = packet_copies(0, x_s)
        g_main, g_tail = packet_copies(1, g_s)
        gate_0, up_0, down_0 = col_copies(0)
        start([x_tail, x_main, gate_0, up_0, g_tail, g_main, down_0] if tail else [x_main, gate_0, up_0, g_main, down_0])
        start(col_copies(1))
        if tail:
            unfold = unfold_matrix(rows, False)
            fold_s[...] = unfold_matrix(rows, True)

        def unpack(n, dst, copy):
            if tail:
                copy.wait()
                opened = dot(unfold, tail_s[n]).astype(BF16)
                for q in range(FOLD):
                    dst[rows : rows + per, q * folded : (q + 1) * folded] = opened[q * per : (q + 1) * per]

        unpack(0, x_s, x_tail)
        wait((x_main, gate_0))
        gate_pre = dot(x_s[...], gate_c[0])
        up_0.wait()
        up_pre = dot(x_s[...], up_c[0])
        unpack(1, g_s, g_tail)
        wait((g_main, down_0))
        hidden_grad = dot_t(g_s[...], down_c[0])
        gg_s[0], ug_s[0] = gradients(gate_pre, up_pre, hidden_grad)

    @pl.when((step > 0) & (step < chunks))
    def _():
        @pl.when(step < chunks - 1)
        def _():
            start(col_copies(step + 1))

        @pl.when(step == chunks - 1)
        def _():
            start(row_copies(0))
            start(row_copies(1))

        wait(col_copies(step))
        slot = step % 2
        gate_pre = dot(x_s[...], gate_c[slot])
        up_pre = dot(x_s[...], up_c[slot])
        hidden_grad = dot_t(g_s[...], down_c[slot])
        gg_s[step], ug_s[step] = gradients(gate_pre, up_pre, hidden_grad)

    @pl.when((step >= chunks) & (step < chunks + blocks))
    def _():
        q = step - chunks
        slot = q % 2
        wait(row_copies(q))
        gg = jnp.concatenate([gg_s[c] for c in range(chunks)], 1)
        ug = jnp.concatenate([ug_s[c] for c in range(chunks)], 1)
        back = (dot_t(gg, gate_r[slot]) + dot_t(ug, up_r[slot])).astype(BF16)
        out_ref[...] = back[0:rows]
        if tail:
            late_s[q] = back[rows:]

        @pl.when(q < blocks - 2)
        def _():
            start(row_copies(q + 2))

    if tail:

        @pl.when(step >= chunks + BLOCKS)
        def _():
            b = step - chunks - BLOCKS
            stacked = jnp.concatenate([late_s[q * (BLOCKS // FOLD) + b] for q in range(FOLD)], 0)
            out_ref[...] = dot(fold_s[...], stacked).astype(BF16)


def expert_backward(packets, gate, up, down, tail, width):
    features, hidden = gate.shape
    rows = packets.shape[0]
    late = rows // FOLD if tail else 0
    folded = features // FOLD if tail else 0
    blocks = BLOCKS if tail else 7
    wide, chunks = features // blocks, hidden // width
    scratch = [
        pltpu.VMEM((rows + late, features), BF16),
        pltpu.VMEM((rows + late, features), BF16),
        pltpu.VMEM((2, features, width), BF16),
        pltpu.VMEM((2, features, width), BF16),
        pltpu.VMEM((2, width, features), BF16),
        pltpu.VMEM((2, wide, hidden), BF16),
        pltpu.VMEM((2, wide, hidden), BF16),
        pltpu.VMEM((chunks, rows + late, width), BF16),
        pltpu.VMEM((chunks, rows + late, width), BF16),
        pltpu.SemaphoreType.DMA((4,)),
        pltpu.SemaphoreType.DMA((3, 2)),
        pltpu.SemaphoreType.DMA((2, 2)),
    ]
    if tail:
        scratch += [
            pltpu.VMEM((2, rows, folded), BF16),
            pltpu.VMEM((rows, rows), BF16),
            pltpu.VMEM((BLOCKS, late, wide), BF16),
        ]
    return pl.pallas_call(
        lambda *refs: expert_kernel(chunks, tail, *refs),
        grid=(chunks + blocks + folded // wide,),
        in_specs=[ANY_SPEC] * 4,
        out_specs=pl.BlockSpec((rows, wide), lambda s: (0, jnp.maximum(s - chunks, 0))),
        out_shape=jax.ShapeDtypeStruct((rows, features + folded), BF16),
        scratch_shapes=scratch,
        compiler_params=pltpu.CompilerParams(vmem_limit_bytes=60 * 1024 * 1024),
        name="expert_backward",
    )(packets, gate, up, down)


def combine_kernel(main_ref, back_ref, *refs):
    step, half = pl.program_id(0), pl.num_programs(0) // 2
    other_ref, own_ref = refs[-2:]
    tokens = own_ref.shape[0]
    both = dot(main_ref[...], back_ref[...])
    if len(refs) > 2:
        both = both + dot(refs[0][...], refs[1][...])
    total = both[:tokens] + both[tokens:]

    @pl.when(step < half)
    def _():
        other_ref[...] = total.astype(BF16)

    @pl.when(step >= half)
    def _():
        own_ref[...] = total


def combine(core, back, main, late=None):
    rows, tokens = back.shape[0], main.shape[0] // 2
    half = BLOCKS // 2
    wide = back.shape[1] // (BLOCKS if late is None else BLOCKS + BLOCKS // FOLD)
    block = (lambda s: s) if core else (lambda s: (s + half) % BLOCKS)
    in_specs = [pl.BlockSpec(main.shape, lambda s: (0, 0)), pl.BlockSpec((rows, wide), lambda s: (0, block(s)))]
    args = [main, back]
    if late is not None:
        in_specs += [
            pl.BlockSpec((2 * tokens, rows), lambda s: (block(s) // half, 0)),
            pl.BlockSpec((rows, wide), lambda s: (0, BLOCKS + s % half)),
        ]
        args += [late, back]
    return pl.pallas_call(
        combine_kernel,
        grid=(BLOCKS,),
        in_specs=in_specs,
        out_specs=[
            pl.BlockSpec((tokens, wide), lambda s: (0, jnp.minimum(s, half - 1))),
            pl.BlockSpec((tokens, wide), lambda s: (0, jnp.maximum(s - half, 0))),
        ],
        out_shape=[jax.ShapeDtypeStruct((tokens, half * wide), kind) for kind in (BF16, F32)],
        name="combine",
    )(*args)


def exchange(packets, experts):
    parts = packets.reshape(experts, TILE, -1)
    return lax.all_to_all(parts, "ep", split_axis=0, concat_axis=0, tiled=True).reshape(packets.shape)


def share(core, experts, ids, probs, x, g, gate, up, down):
    base, tail = CORES[core]
    packets = dispatch(ids, x, g, experts, base, tail)
    if core == 0:
        arrived = exchange(packets, experts)
    else:
        packets, *weights = weights_and_wait(WAIT, ids, probs, packets, experts, base, tail)
        arrived = exchange(packets, experts)
    returned = exchange(expert_backward(arrived, gate, up, down, tail, WIDTHS[core]), experts)
    if core == 0:
        returned, *weights = weights_and_wait(0, ids, probs, returned, experts, base, tail)
    return tuple(combine(core, returned, *weights))


def body(layer_input, out_grad, expert_ids, gate_probs, gate_proj, up_proj, down_proj):
    experts = lax.axis_size("ep")
    args = (expert_ids.T, gate_probs.T, layer_input, out_grad, gate_proj[0], up_proj[0], down_proj[0])
    paths = [lambda *args, core=core: share(core, experts, *args) for core in (0, 1)]
    crossing, own = lax.cond(lax.axis_index("dp") == 0, *paths, *args)
    return (own + lax.ppermute(crossing, "dp", ((0, 1), (1, 0))).astype(F32)).astype(BF16)


def solution(mesh):
    rows = P("ep", None)
    mats = P("ep", None, None)
    return jax.shard_map(body, mesh=mesh, in_specs=(rows,) * 4 + (mats,) * 3, out_specs=P("ep", "dp"), check_vma=False)
```
